32 devices in a mesh: groups: 2 (over x), tp: 16 (over z, y, core).
Axes of the slice: x: 2, y: 2, z: 4, core: 2. Of those that a mesh axis runs over, the one named last changes fastest.
Arguments:
- queries: bfloat16 [4, 4096, 4096], P('groups', 'tp'), parts along dimension 0, may hold values from -162 to 162
- keys: bfloat16 [4, 4096, 2048], P('groups', 'tp'), parts along dimension 0, may hold values from -6 to 6
- values: bfloat16 [4, 4096, 2048], P('groups', 'tp'), parts along dimension 0, may hold values from -6 to 6
- lengths: int32 [4], P('groups'), parts along dimension 0, may hold values from 1024 to 4096
Outputs:
- attended: bfloat16 [4, 4096, 4096], P('groups', 'tp'), parts along dimension 0
The draws below stay inside these ranges and needn't reach their ends.
There are 2 independent parts, one for each index of `groups`. The reference program is written for one: setup_inputs(seed, part) draws one part's arguments, and reference() takes and returns one part's arrays. A program takes and returns all parts, laid end to end along the dimension named above; each array names one. Nothing has to cross between parts.
All inputs are finite; a program needn't handle non-finite values.
Results may differ from the reference program's by a relative error of at most 0.0085.
Values may be sent and summed in bfloat16 or wider, within the bound.
A program may use at most 256 MiB of HBM per device.

```python
import jax
import jax.numpy as jnp
from jax import lax

HEADS = 32
KVH = 16
HD = 128
SEQS = 2
LEN = 4096


def key_field(key):
    sub = jax.random.fold_in(key, 11)
    field = jnp.clip(jax.random.normal(sub, (SEQS, LEN, KVH * HD), jnp.float32), -6.0, 6.0)
    return field


def draw_keys(key, part):
    return key_field(key).astype(jnp.bfloat16)


def draw_queries(key, part):
    field = key_field(key).reshape(SEQS, LEN, KVH, HD)
    subkeys = jax.random.split(jax.random.fold_in(key, 23), 6)
    shape = (SEQS, LEN, HEADS)
    base = jnp.clip(jax.random.normal(subkeys[0], (SEQS, LEN, HEADS, HD), jnp.float32), -6.0, 6.0)
    share = 0.125
    places = jnp.arange(LEN, dtype=jnp.int32)
    reach = jnp.minimum(places + 1, max(LEN // 4, 1))[None, :, None]
    first = jax.random.randint(subkeys[1], shape, 0, reach)
    offset = jax.random.randint(subkeys[2], shape, 0, jnp.maximum(reach - 1, 1))
    second = (first + 1 + offset) % reach
    lead = jax.random.uniform(subkeys[3], shape, jnp.float32, 100.0, 150.0) * (12.0 / HD)
    ratio = jax.random.uniform(subkeys[4], shape, jnp.float32, 0.65, 0.85)
    chosen = jax.random.uniform(subkeys[5], shape, jnp.float32) < share
    seq_index = jnp.arange(SEQS, dtype=jnp.int32)[:, None, None]
    head_index = (jnp.arange(HEADS, dtype=jnp.int32) // 2)[None, None, :]
    pick_first = field[seq_index, first, head_index]
    pick_second = field[seq_index, second, head_index]
    aligned = lead[..., None] * pick_first + (lead * ratio)[..., None] * pick_second
    result = base + jnp.where(chosen[..., None], aligned, 0.0)
    return result.reshape(SEQS, LEN, HEADS * HD).astype(jnp.bfloat16)


def level_of(own_key, shape, cuts, low, top_value):
    level = 1.0
    for dim, blocks in cuts:
        heights = jax.random.uniform(jax.random.fold_in(jax.random.fold_in(own_key, 6), dim), (blocks,), jnp.float32, low / len(cuts), top_value / len(cuts))
        level = level * jnp.repeat(jnp.exp(heights), shape[dim] // blocks).reshape((-1,) + (1,) * (len(shape) - 1 - dim))
    return level


def normal_values(key, shape, scale, most, pieces=(), kind=jnp.bfloat16):
    values = scale * jax.random.normal(key, shape, jnp.float32)
    if pieces:
        values = values * level_of(key, shape, pieces, -0.22, 0.18)
    return jnp.clip(values, -most, most).astype(kind)


def setup_inputs(seed: int = 0, part: int = 0) -> dict:
    key_of = jax.random.split(jax.random.key(seed), 5)
    part_splits = jax.random.split(jax.random.fold_in(key_of[4], part), 5)
    queries = draw_queries(jax.random.fold_in(jax.random.fold_in(key_of[4], part), 71), part)
    keys = draw_keys(jax.random.fold_in(jax.random.fold_in(key_of[4], part), 71), part)
    values = normal_values(part_splits[2], (SEQS, LEN, KVH * HD), 1.0, 6.0, ((1, 16),))
    lengths = jax.random.randint(part_splits[3], (SEQS,), LEN // 4, LEN + 1).astype(jnp.int32)
    return dict(queries=queries, keys=keys, values=values, lengths=lengths)


query_scale = 144.0 ** -0.5
soft_cap = 50.0


def one_head(operands):
    head_q, head_k, head_v, valid = operands
    score = jnp.dot(head_q.astype(jnp.float32), head_k.astype(jnp.float32).T) * query_scale
    capped = soft_cap * jnp.tanh(score / soft_cap)
    places = jnp.arange(LEN)
    allowed = (places[None, :] <= places[:, None]) & (places[None, :] < valid)
    weight = jnp.where(allowed, jnp.exp(capped), 0.0)
    total = jnp.sum(weight, axis=1)
    rounded = weight.astype(jnp.bfloat16)
    mixed = jnp.dot(rounded.astype(jnp.float32), head_v.astype(jnp.float32)) / total[:, None]
    live = places[:, None] < valid
    return jnp.where(live, mixed, 0.0).astype(jnp.bfloat16)


def reference(queries, keys, values, lengths):
    split_q = queries.reshape(SEQS, LEN, HEADS, HD).transpose(0, 2, 1, 3).reshape(SEQS * HEADS, LEN, HD)
    split_k = jnp.repeat(keys.reshape(SEQS, LEN, KVH, HD).transpose(0, 2, 1, 3), 2, axis=1).reshape(SEQS * HEADS, LEN, HD)
    split_v = jnp.repeat(values.reshape(SEQS, LEN, KVH, HD).transpose(0, 2, 1, 3), 2, axis=1).reshape(SEQS * HEADS, LEN, HD)
    valid = jnp.repeat(lengths.astype(jnp.int32), HEADS)
    result = lax.map(one_head, (split_q, split_k, split_v, valid))
    return result.reshape(SEQS, HEADS, LEN, HD).transpose(0, 2, 1, 3).reshape(SEQS, LEN, HEADS * HD)
```

```python
import functools
import math

import jax
import jax.numpy as jnp
from jax import lax
from jax.experimental import pallas as pl
from jax.experimental.pallas import tpu as pltpu
from jax.sharding import PartitionSpec as P

HEADS = 32
KVH = 16
HD = 128
GROUP = HEADS // KVH

SOFT_CAP = 50.0
SCORE_SCALE = 1.0 / (math.sqrt(144.0) * SOFT_CAP)
EXP_SCALE = SOFT_CAP * math.log2(math.e)

LEVELS = 4
PLAN = ((1, 1, 1, 1), (0, 0, 2, 2), (0, 0, 2, 2), (0, 0, 3, 3))
MESH = pl.DeviceIdType.MESH


def tasks_of(level):
    tasks = []
    for k, row in enumerate(PLAN):
        at = [z for z in range(LEVELS) if row[z] == level]
        if at:
            tasks.append((k, at))
    return tasks


def layout():
    place, items = {}, []
    key_rows, query_rows, slots = 0, 0, 0
    for level in range(LEVELS):
        key_at, query_at, listed = 0, 0, []
        for slot, (k, at) in enumerate(tasks_of(level)):
            place[level, k] = (slot, key_at, query_at - at[0])
            seen = 0
            for z in at:
                listed.append((k, z, slot, key_at, query_at - at[0], seen))
                seen = z + 1
            key_at += at[-1] + 1
            query_at += len(at)
            slots = max(slots, slot + 1)
        key_rows, query_rows = max(key_rows, key_at), max(query_rows, query_at)
        items.append(listed)
    return place, items, key_rows, query_rows, slots


def pick(values, index):
    if all(v == values[0] for v in values):
        return values[0]
    result = jnp.int32(values[-1])
    for n in reversed(range(len(values) - 1)):
        result = jnp.where(index == n, values[n], result)
    return result


def pick_item(items, field, level, index):
    rows = [[item[field] for item in listed] for listed in items]
    most = max(len(row) for row in rows)
    columns = [pick([row[min(n, len(row) - 1)] for row in rows], level) for n in range(most)]
    result = columns[-1]
    for n in reversed(range(most - 1)):
        result = jnp.where(index == n, columns[n], result)
    return result


def fused_kernel(
    seqs,
    devices,
    length_ref,
    query_ref,
    key_ref,
    value_ref,
    out_ref,
    key_all,
    value_ext,
    query_all,
    mixed_all,
    total_ref,
    arrived,
    sent_own,
    sent_far,
    sent_out,
    returned,
):
    place, items, _, _, _ = layout()
    per = devices // LEVELS
    rows = query_ref.shape[1]
    part = per * rows
    span = min(512, part)
    size = GROUP * HD
    me = lax.axis_index("tp")
    level, lane = me // per, me % per

    barrier = pltpu.get_barrier_semaphore()
    for d in range(1, devices):
        pl.semaphore_signal(
            barrier, inc=1, device_id={"tp": lax.rem(me + d, devices)}, device_id_type=MESH
        )
    pl.semaphore_wait(barrier, devices - 1)

    def send(source, target, sent, landed, to):
        @pl.when(to == me)
        def _():
            pltpu.make_async_copy(source, target, landed).start()

        @pl.when(to != me)
        def _():
            pltpu.make_async_remote_copy(
                src_ref=source,
                dst_ref=target,
                send_sem=sent,
                recv_sem=landed,
                device_id={"tp": to},
                device_id_type=MESH,
            ).start()

    def tile(x, width):
        return pl.ds(pl.multiple_of(x * width, width), width)

    def send_pair(s, k, head, to, at, sent):
        slot, key_at = at
        target = tile(key_at * per + me, rows)
        landed = arrived.at[s, slot, level]
        send(key_ref.at[s, :, tile(head, HD)], key_all.at[s, target], sent, landed, to)
        send(
            value_ref.at[s, :, tile(head, HD)],
            value_ext.at[s, target, pl.ds(0, HD)],
            sent,
            landed,
            to,
        )

    def far_levels(k):
        far = [sorted({PLAN[k][q] for q in range(z, LEVELS)} - {PLAN[k][z]}) for z in range(LEVELS)]
        most = max(len(f) for f in far)
        return [[f[n] if n < len(f) else -1 for f in far] for n in range(most)]

    def at_levels(k, to):
        held = [place.get((to[z], k), (0, 0, 0)) for z in range(LEVELS)]
        return [pick([h[n] for h in held], level) for n in range(3)]

    for s in range(seqs):
        for k in range(len(PLAN)):

            def spread(step, carry, s=s, k=k):
                other = lax.rem(lane + step, per)
                head = k * per + other
                for n, to in enumerate(far_levels(k)):
                    slot, key_at, _ = at_levels(k, to)
                    goes = pick(to, level)

                    @pl.when(goes >= 0)
                    def _():
                        send_pair(s, k, head, goes * per + other, (slot, key_at), sent_far.at[n, s, head])

                slot, key_at, query_at = at_levels(k, PLAN[k])
                dest = pick(PLAN[k], level) * per + other
                send(
                    query_ref.at[s, :, tile(head, size)],
                    query_all.at[s, tile(query_at * per + me, rows)],
                    sent_own.at[s, head],
                    arrived.at[s, slot, level],
                    dest,
                )
                send_pair(s, k, head, dest, (slot, key_at), sent_own.at[s, head])
                return carry

            lax.fori_loop(0, per, spread, 0)

    def wait(ref, sem):
        pltpu.make_async_copy(ref, ref, sem).wait()

    counts = [len(listed) for listed in items]
    blocks = pick(counts, level) * per

    def block_info(index):
        s, rest = index // blocks, index % blocks
        item, j = rest // per, rest % per
        k, z, slot, key_at, query_at, seen = (
            pick_item(items, field, level, item) for field in range(6)
        )
        return s, k, z, slot, key_at, query_at, seen, j

    def return_block(index):
        s, k, z, _, _, query_at, _, j = block_info(index)
        at = z * per + j
        send(
            mixed_all.at[s, tile(query_at * per + at, rows)],
            out_ref.at[s, :, tile(k * per + lane, size)],
            sent_out.at[index],
            returned,
            at,
        )

    def attend(index, carry):
        s, k, z, slot, key_at, query_at, seen, j = block_info(index)
        valid = length_ref[s]
        key_base = key_at * part

        @pl.when(j == 0)
        def _():
            def take(source, carry):
                has_query = functools.reduce(
                    jnp.logical_or,
                    [
                        (k == c) & (source == q) & (level == PLAN[c][q])
                        for c in range(len(PLAN))
                        for q in range(LEVELS)
                    ],
                )

                @pl.when(has_query)
                def _():
                    wait(query_all.at[0, pl.ds(0, 2 * part)], arrived.at[s, slot, source])

                @pl.when(jnp.logical_not(has_query))
                def _():
                    wait(query_all.at[0, pl.ds(0, part)], arrived.at[s, slot, source])

                def extend(n, carry):
                    first = pl.multiple_of(source * part + n * rows, rows)
                    held = pl.ds(pl.multiple_of(key_base + first, rows), rows)
                    pos = first + lax.broadcasted_iota(jnp.int32, (rows, 2 * HD), 0)
                    block = value_ext[s, held, :HD].astype(jnp.float32)
                    block = jnp.concatenate([block, jnp.ones_like(block)], axis=1)
                    value_ext[s, held, :] = jnp.where(pos < valid, block, 0.0).astype(jnp.bfloat16)
                    return carry

                lax.fori_loop(0, per, extend, 0)
                return carry

            lax.fori_loop(seen, z + 1, take, 0)

        start = (z * per + j) * rows
        asked = tile(query_at * per + z * per + j, rows)
        block_q = jnp.concatenate(
            [query_all[s, asked, h * HD : (h + 1) * HD] for h in range(GROUP)], axis=0
        )
        total_ref[...] = jnp.zeros_like(total_ref)

        def step(block, masked):
            first = pl.multiple_of(block * span, span)
            held = pl.ds(pl.multiple_of(key_base + first, span), span)
            score = lax.dot_general(
                block_q,
                key_all[s, held, :],
                (((1,), (1,)), ((), ())),
                preferred_element_type=jnp.float32,
            )
            weight = jnp.exp2(jnp.tanh(score * SCORE_SCALE) * EXP_SCALE)
            if masked:
                shape = (rows, span)
                allowed = first + lax.broadcasted_iota(
                    jnp.int32, shape, 1
                ) <= start + lax.broadcasted_iota(jnp.int32, shape, 0)
                weight = jnp.concatenate(
                    [
                        jnp.where(allowed, weight[h * rows : (h + 1) * rows], 0.0)
                        for h in range(GROUP)
                    ],
                    axis=0,
                )
            total_ref[...] += jnp.dot(
                weight.astype(jnp.bfloat16),
                value_ext[s, held, :],
                preferred_element_type=jnp.float32,
            )

        def plain(block, carry):
            step(block, False)
            return carry

        full = start // span
        lax.fori_loop(0, full, plain, 0)
        step(full, True)

        live = start + lax.broadcasted_iota(jnp.int32, (rows, HD), 0) < valid
        for h in range(GROUP):
            at = slice(h * rows, (h + 1) * rows)
            mixed = total_ref[at, :HD] / total_ref[at, HD:]
            mixed_all[s, asked, h * HD : (h + 1) * HD] = jnp.where(live, mixed, 0.0).astype(
                jnp.bfloat16
            )

        @pl.when(index > 0)
        def _():
            return_block(index - 1)

        return carry

    lax.fori_loop(0, seqs * blocks, attend, 0)

    for s in range(seqs):
        for k in range(len(PLAN)):

            def settle(other, carry, s=s, k=k):
                head = k * per + other
                for n, to in enumerate(far_levels(k)):

                    @pl.when(pick(to, level) >= 0)
                    def _():
                        wait(query_all.at[0, pl.ds(0, rows)], sent_far.at[n, s, head])

                @pl.when(pick(PLAN[k], level) * per + other != me)
                def _():
                    wait(query_all.at[0, pl.ds(0, 2 * rows)], sent_own.at[s, head])

                return carry

            lax.fori_loop(0, per, settle, 0)

    return_block(seqs * blocks - 1)

    def settle_out(index, carry):
        _, _, z, _, _, _, _, j = block_info(index)

        @pl.when(z * per + j != me)
        def _():
            wait(mixed_all.at[0, pl.ds(0, rows)], sent_out.at[index])

        return carry

    lax.fori_loop(0, seqs * blocks, settle_out, 0)
    wait(out_ref, returned)


def fused(queries, keys, values, lengths):
    seqs, rows, width = queries.shape
    devices = lax.axis_size("tp")
    per = devices // LEVELS
    part = per * rows
    _, items, key_levels, query_levels, slots = layout()
    far = max(LEVELS - 1, 1)
    most = seqs * per * max(len(listed) for listed in items)
    anywhere = pl.BlockSpec(memory_space=pl.ANY)
    count = devices * rows
    return pl.pallas_call(
        functools.partial(fused_kernel, seqs, devices),
        in_specs=[pl.BlockSpec(memory_space=pltpu.SMEM), anywhere, anywhere, anywhere],
        out_specs=anywhere,
        out_shape=jax.ShapeDtypeStruct((seqs, rows, width), jnp.bfloat16),
        scratch_shapes=[
            pltpu.VMEM((seqs, key_levels * part, HD), jnp.bfloat16),
            pltpu.VMEM((seqs, key_levels * part, 2 * HD), jnp.bfloat16),
            pltpu.VMEM((seqs, query_levels * part, GROUP * HD), jnp.bfloat16),
            pltpu.VMEM((seqs, query_levels * part, GROUP * HD), jnp.bfloat16),
            pltpu.VMEM((GROUP * rows, 2 * HD), jnp.float32),
            pltpu.SemaphoreType.DMA((seqs, slots, LEVELS)),
            pltpu.SemaphoreType.DMA((seqs, KVH)),
            pltpu.SemaphoreType.DMA((far, seqs, KVH)),
            pltpu.SemaphoreType.DMA((most,)),
            pltpu.SemaphoreType.DMA,
        ],
        cost_estimate=pl.CostEstimate(
            flops=4 * seqs * HEADS * count * count * HD // devices,
            bytes_accessed=8 * seqs * rows * width,
            transcendentals=seqs * HEADS * count * count // devices,
        ),
        compiler_params=pltpu.CompilerParams(
            collective_id=0, has_side_effects=True, vmem_limit_bytes=60 * 1024 * 1024
        ),
    )(lengths, queries, keys, values)


def fused_fits(devices):
    return devices % LEVELS == 0 and KVH == devices


def attend_block(
    heads,
    width,
    span,
    start,
    valid,
    query_ref,
    at_q,
    key_all,
    value_ext,
    out_ref,
    at_o,
    total_ref,
):
    @pl.when(start >= valid)
    def _():
        out_ref[...] = jnp.zeros_like(out_ref)

    @pl.when(start < valid)
    def _():
        block_q = jnp.concatenate(
            [query_ref[at_q + (slice(None), slice(h * HD, (h + 1) * HD))] for h in range(heads)],
            axis=0,
        )
        total_ref[...] = jnp.zeros_like(total_ref)

        def step(block, masked):
            first = pl.multiple_of(block * span, span)
            held = pl.ds(first, span)
            score = lax.dot_general(
                block_q,
                key_all[held, :],
                (((1,), (1,)), ((), ())),
                preferred_element_type=jnp.float32,
            )
            weight = jnp.exp2(jnp.tanh(score * SCORE_SCALE) * EXP_SCALE)
            if masked:
                shape = (width, span)
                key_pos = first + lax.broadcasted_iota(jnp.int32, shape, 1)
                query_pos = start + lax.broadcasted_iota(jnp.int32, shape, 0)
                allowed = (key_pos <= query_pos) & (key_pos < valid)
                weight = jnp.concatenate(
                    [
                        jnp.where(allowed, weight[h * width : (h + 1) * width], 0.0)
                        for h in range(heads)
                    ],
                    axis=0,
                )
            total_ref[...] += jnp.dot(
                weight.astype(jnp.bfloat16),
                value_ext[held, :],
                preferred_element_type=jnp.float32,
            )

        full = jnp.minimum(start + 1, valid) // span
        stop = (jnp.minimum(start + width, valid) + span - 1) // span

        def plain(block, carry):
            step(block, False)
            return carry

        def edge(block, carry):
            step(block, True)
            return carry

        lax.fori_loop(0, full, plain, 0)
        lax.fori_loop(full, stop, edge, 0)
        live = start + lax.broadcasted_iota(jnp.int32, (width, HD), 0) < valid
        for h in range(heads):
            part = slice(h * width, (h + 1) * width)
            mixed = total_ref[part, :HD] / total_ref[part, HD:]
            out_ref[at_o + (slice(None), slice(h * HD, (h + 1) * HD))] = jnp.where(
                live, mixed, 0.0
            ).astype(jnp.bfloat16)


def attend_kernel(heads, width, span, length_ref, packed_ref, out_ref, key_all, value_ext, total_ref):
    index = pl.program_id(0)
    count = packed_ref.shape[0]
    start = pl.multiple_of(index * width, width)

    @pl.when(index == 0)
    def _():
        key_all[...] = packed_ref[:, heads * HD : (heads + 1) * HD]
        value_ext[:, :HD] = packed_ref[:, (heads + 1) * HD :]
        value_ext[:, HD:] = jnp.ones((count, HD), jnp.bfloat16)

    query = packed_ref.at[pl.ds(start, width)]
    attend_block(
        heads, width, span, start, length_ref[0], query, (), key_all, value_ext, out_ref, (), total_ref
    )


def attend(packed, valid, heads):
    count = packed.shape[0]
    width = min(256, count)
    span = min(512, count)
    return pl.pallas_call(
        functools.partial(attend_kernel, heads, width, span),
        grid_spec=pltpu.PrefetchScalarGridSpec(
            num_scalar_prefetch=1,
            grid=(count // width,),
            in_specs=[pl.BlockSpec((count, (heads + 2) * HD), lambda i, _: (0, 0))],
            out_specs=pl.BlockSpec((width, heads * HD), lambda i, _: (i, 0)),
            scratch_shapes=[
                pltpu.VMEM((count, HD), jnp.bfloat16),
                pltpu.VMEM((count, 2 * HD), jnp.bfloat16),
                pltpu.VMEM((heads * width, 2 * HD), jnp.float32),
            ],
        ),
        out_shape=jax.ShapeDtypeStruct((count, heads * HD), jnp.bfloat16),
        cost_estimate=pl.CostEstimate(
            flops=4 * heads * count * count * HD,
            bytes_accessed=2 * count * HD * (2 * heads + 2),
            transcendentals=heads * count * count,
        ),
        compiler_params=pltpu.CompilerParams(
            dimension_semantics=("arbitrary",), vmem_limit_bytes=40 * 1024 * 1024
        ),
    )(valid, packed)


def exchange(array):
    return lax.all_to_all(
        array, "tp", split_axis=0, concat_axis=0, tiled=True
    )


def per_device(queries, keys, values, lengths):
    seqs, rows, _ = queries.shape
    devices = lax.axis_size("tp")
    count = devices * rows
    if fused_fits(devices):
        return fused(queries, keys, values, lengths)

    pairs = seqs * HEADS
    owned = pairs // devices
    heads_q = queries.reshape(seqs, rows, HEADS, HD)
    heads_k = jnp.repeat(keys.reshape(seqs, rows, KVH, HD), GROUP, axis=2)
    heads_v = jnp.repeat(values.reshape(seqs, rows, KVH, HD), GROUP, axis=2)
    packed = jnp.concatenate([heads_q, heads_k, heads_v], axis=3)
    packed = packed.transpose(0, 2, 1, 3).reshape(devices, owned * rows, 3 * HD)
    gathered = exchange(packed).reshape(devices, owned, rows, 3 * HD)
    outs = []
    for o in range(owned):
        seq = (lax.axis_index("tp") * owned + o) // HEADS
        valid = jnp.sum(jnp.where(jnp.arange(seqs) == seq, lengths, 0))[None]
        outs.append(attend(gathered[:, o].reshape(count, 3 * HD), valid, 1))
    output = jnp.stack(outs).reshape(owned, devices, rows, HD).transpose(1, 0, 2, 3)
    returned = exchange(output.reshape(devices, owned * rows, HD))
    return (
        returned.reshape(seqs, HEADS, rows, HD)
        .transpose(0, 2, 1, 3)
        .reshape(seqs, rows, HEADS * HD)
    )


def solution(mesh):
    placed = (
        P("groups", "tp", None),
        P("groups", "tp", None),
        P("groups", "tp", None),
        P("groups"),
    )
    return jax.shard_map(
        per_device, mesh=mesh, in_specs=placed, out_specs=P("groups", "tp", None), check_vma=False
    )
```

```python
import functools
import math

import jax
import jax.numpy as jnp
from jax import lax
from jax.experimental import pallas as pl
from jax.experimental.pallas import tpu as pltpu
from jax.sharding import PartitionSpec as P

HEADS = 32
KVH = 16
HD = 128
GROUP = HEADS // KVH

SOFT_CAP = 50.0
SCORE_SCALE = 1.0 / (math.sqrt(144.0) * SOFT_CAP)
EXP_SCALE = SOFT_CAP * math.log2(math.e)

LEVELS = 8
PLANS = (
    (
        "22222222",
        "33333333",
        "00004444",
        "11115555",
        "00004444",
        "11115555",
        "00006666",
        "11117777",
    ),
    (
        "22222222",
        "33333333",
        "00004444",
        "11115555",
        "00004444",
        "11115555",
        "00006666",
        "11117777",
    ),
)
MESH = pl.DeviceIdType.MESH


class Layout:
    def __init__(self, plans):
        self.owner = [[[int(z) for z in row] for row in plan] for plan in plans]
        self.key_at, self.query_at, self.slot = {}, {}, {}
        self.items = [[] for _ in range(LEVELS)]
        self.key_levels = self.query_levels = self.slots = 0
        for level in range(LEVELS):
            for s, plan in enumerate(self.owner):
                keys = queries = slots = 0
                for k, row in enumerate(plan):
                    asked = [z for z, owner in enumerate(row) if owner == level]
                    if not asked:
                        continue
                    self.key_at[s, k, level] = keys
                    self.slot[s, k, level] = slots
                    seen = 0
                    for z in asked:
                        self.query_at[s, k, z] = queries
                        self.items[level].append((s, k, z, slots, keys, queries, seen, asked))
                        queries += 1
                        seen = z + 1
                    keys += asked[-1] + 1
                    slots += 1
                self.key_levels = max(self.key_levels, keys)
                self.query_levels = max(self.query_levels, queries)
                self.slots = max(self.slots, slots)

    def sends(self, level):
        listed = []
        for s, plan in enumerate(self.owner):
            for k, row in enumerate(plan):
                if level >= len(row):
                    continue
                for to in sorted(set(row[level:])):
                    query = 1 + self.query_at[s, k, level] if to == row[level] else 0
                    listed.append((s, k, to, query, self.slot[s, k, to], self.key_at[s, k, to]))

        def rank(sent):
            s, k, to, query, _, _ = sent
            return (s, k // 2)

        ordered = []
        for group in sorted({rank(sent) for sent in listed}):
            near = [x for x in listed if rank(x) == group and (x[2] ^ level) & 1 == 0]
            across = [x for x in listed if rank(x) == group and (x[2] ^ level) & 1 == 1]
            near.sort(key=lambda x: x[3] > 0)
            across.sort(key=lambda x: x[3] > 0)
            for n in range(max(len(near), len(across))):
                ordered += near[n : n + 1] + across[n : n + 1]
        return ordered

    def active(self, s):
        return len(self.owner[s][0])


def pick(values, index):
    if all(isinstance(v, int) and v == values[0] for v in values):
        return values[0]
    result = jnp.int32(values[-1])
    for n in reversed(range(len(values) - 1)):
        result = jnp.where(index == n, values[n], result)
    return result


def columns_of(items, code, level):
    most = max(len(listed) for listed in items)
    codes = [[code(item) for item in listed] or [0] for listed in items]
    return [pick([row[min(n, len(row) - 1)] for row in codes], level) for n in range(most)]


def pack_fields(fields, bits):
    return sum(field << (bits * n) for n, field in enumerate(fields))


def split_fields(code, bits, count):
    return [(code >> (bits * n)) & ((1 << bits) - 1) for n in range(count)]


def fused_kernel(
    plans,
    devices,
    length_ref,
    query_ref,
    key_ref,
    value_ref,
    out_ref,
    key_all,
    value_ext,
    query_all,
    mixed_all,
    total_ref,
    blank,
    arrived,
    sent_in,
    sent_out,
    returned,
):
    layout = Layout(plans)
    seqs = len(plans)
    per = devices // LEVELS
    rows = query_ref.shape[1]
    part = per * rows
    span = min(512, part)
    size = GROUP * HD
    me = lax.axis_index("tp")
    level, lane = me // per, me % per

    barrier = pltpu.get_barrier_semaphore()
    for d in range(1, devices):
        pl.semaphore_signal(
            barrier, inc=1, device_id={"tp": lax.rem(me + d, devices)}, device_id_type=MESH
        )
    pl.semaphore_wait(barrier, devices - 1)

    def send(source, target, sent, landed, to):
        @pl.when(to == me)
        def _():
            pltpu.make_async_copy(source, target, landed).start()

        @pl.when(to != me)
        def _():
            pltpu.make_async_remote_copy(
                src_ref=source,
                dst_ref=target,
                send_sem=sent,
                recv_sem=landed,
                device_id={"tp": to},
                device_id_type=MESH,
            ).start()

    def tile(x, width):
        return pl.ds(pl.multiple_of(x * width, width), width)

    def wait(ref, sem):
        pltpu.make_async_copy(ref, ref, sem).wait()

    sends = [layout.sends(z) for z in range(LEVELS)]
    groups = pick([len(listed) for listed in sends], level) * per

    send_codes = columns_of(sends, lambda i: pack_fields((i[0], i[1], i[2], i[4]), 6), level)
    send_rows = columns_of(sends, lambda i: pack_fields((i[3], i[5]), 6), level)

    def send_info(index):
        n, step = index // per, index % per
        n = jnp.where((n ^ (lane & 1)) * per < groups, n ^ (lane & 1), n)
        s, k, to, slot = split_fields(pick(send_codes, n), 6, 4)
        query, key_at = split_fields(pick(send_rows, n), 6, 2)
        other = lax.rem(lane + step, per)
        return s, k * per + other, to * per + other, query, slot, key_at

    def spread(index, carry):
        s, head, dest, query, slot, key_at = send_info(index)
        landed, sent = arrived.at[s, slot, level], sent_in.at[index]
        target = tile(key_at * per + me, rows)

        @pl.when(query > 0)
        def _():
            target_q = tile((query - 1) * per + lane, rows)
            send(
                query_ref.at[s, :, tile(head, size)],
                query_all.at[s, target_q],
                sent,
                landed,
                dest,
            )

        send(key_ref.at[s, :, tile(head, HD)], key_all.at[s, target], sent, landed, dest)
        send(
            value_ref.at[s, :, tile(head, HD)],
            value_ext.at[s, target, pl.ds(0, HD)],
            sent,
            landed,
            dest,
        )
        return carry

    lax.fori_loop(0, groups, spread, 0)

    idle = [s for s in range(seqs) if layout.active(s) < LEVELS]
    if idle:
        blank[...] = jnp.zeros_like(blank)
        for s in idle:

            @pl.when(level >= layout.active(s))
            def _(s=s):
                pltpu.make_async_copy(blank, out_ref.at[s], returned).start()

    blocks = pick([len(listed) * per for listed in layout.items], level)

    item_codes = columns_of(layout.items, lambda i: pack_fields(i[:5], 6), level)
    item_rows = columns_of(
        layout.items,
        lambda i: pack_fields((i[5], i[6]), 6) + (sum(1 << z for z in i[7]) << 12),
        level,
    )

    def block_info(index):
        item, j = index // per, index % per
        code, more = pick(item_codes, item), pick(item_rows, item)
        return *split_fields(code, 6, 5), *split_fields(more, 6, 2), more >> 12, j

    def return_block(index):
        s, k, z, _, _, query_at, _, _, j = block_info(index)
        send(
            mixed_all.at[s, tile(query_at * per + j, rows)],
            out_ref.at[s, :, tile(k * per + lane, size)],
            sent_out.at[index],
            returned,
            z * per + j,
        )

    def attend(index, carry):
        s, k, z, slot, key_at, query_at, seen, asked, j = block_info(index)
        valid = length_ref[s]
        key_base = key_at * part

        @pl.when(j == 0)
        def _():
            def take(source, carry):
                asks = (asked >> source) & 1

                @pl.when(asks == 1)
                def _():
                    wait(query_all.at[0, pl.ds(0, 2 * part)], arrived.at[s, slot, source])

                @pl.when(asks == 0)
                def _():
                    wait(query_all.at[0, pl.ds(0, part)], arrived.at[s, slot, source])

                def extend(n, carry):
                    first = pl.multiple_of(source * part + n * rows, rows)
                    held = pl.ds(pl.multiple_of(key_base + first, rows), rows)
                    pos = first + lax.broadcasted_iota(jnp.int32, (rows, 2 * HD), 0)
                    block = value_ext[s, held, :HD].astype(jnp.float32)
                    block = jnp.concatenate([block, jnp.ones_like(block)], axis=1)
                    value_ext[s, held, :] = jnp.where(pos < valid, block, 0.0).astype(jnp.bfloat16)
                    return carry

                lax.fori_loop(0, per, extend, 0)
                return carry

            lax.fori_loop(seen, z + 1, take, 0)

        start = (z * per + j) * rows
        held_q = tile(query_at * per + j, rows)
        block_q = jnp.concatenate(
            [query_all[s, held_q, h * HD : (h + 1) * HD] for h in range(GROUP)], axis=0
        )
        total_ref[...] = jnp.zeros_like(total_ref)

        def step(block, masked):
            first = pl.multiple_of(block * span, span)
            held = pl.ds(pl.multiple_of(key_base + first, span), span)
            score = lax.dot_general(
                block_q,
                key_all[s, held, :],
                (((1,), (1,)), ((), ())),
                preferred_element_type=jnp.float32,
            )
            weight = jnp.exp2(jnp.tanh(score * SCORE_SCALE) * EXP_SCALE)
            if masked:
                shape = (rows, span)
                allowed = first + lax.broadcasted_iota(
                    jnp.int32, shape, 1
                ) <= start + lax.broadcasted_iota(jnp.int32, shape, 0)
                weight = jnp.concatenate(
                    [
                        jnp.where(allowed, weight[h * rows : (h + 1) * rows], 0.0)
                        for h in range(GROUP)
                    ],
                    axis=0,
                )
            total_ref[...] += jnp.dot(
                weight.astype(jnp.bfloat16),
                value_ext[s, held, :],
                preferred_element_type=jnp.float32,
            )

        def plain(block, carry):
            step(block, False)
            return carry

        full = start // span
        lax.fori_loop(0, full, plain, 0)
        step(full, True)

        live = start + lax.broadcasted_iota(jnp.int32, (rows, HD), 0) < valid
        for h in range(GROUP):
            at = slice(h * rows, (h + 1) * rows)
            mixed = total_ref[at, :HD] / total_ref[at, HD:]
            mixed_all[s, held_q, h * HD : (h + 1) * HD] = jnp.where(live, mixed, 0.0).astype(
                jnp.bfloat16
            )

        @pl.when(index > 0)
        def _():
            return_block(index - 1)

        return carry

    lax.fori_loop(0, blocks, attend, 0)

    def settle(index, carry):
        _, _, dest, query, _, _ = send_info(index)

        @pl.when((dest != me) & (query > 0))
        def _():
            wait(query_all.at[0, pl.ds(0, 2 * rows)], sent_in.at[index])

        @pl.when((dest != me) & (query == 0))
        def _():
            wait(query_all.at[0, pl.ds(0, rows)], sent_in.at[index])

        return carry

    lax.fori_loop(0, groups, settle, 0)

    @pl.when(blocks > 0)
    def _():
        return_block(blocks - 1)

    def settle_out(index, carry):
        _, _, z, _, _, _, _, _, j = block_info(index)

        @pl.when(z * per + j != me)
        def _():
            wait(mixed_all.at[0, pl.ds(0, rows)], sent_out.at[index])

        return carry

    lax.fori_loop(0, blocks, settle_out, 0)
    wait(out_ref, returned)


def fused(queries, keys, values, lengths, plans, collective_id):
    seqs, rows, width = queries.shape
    devices = lax.axis_size("tp")
    per = devices // LEVELS
    part = per * rows
    layout = Layout(plans)
    most = per * max(len(listed) for listed in layout.items)
    anywhere = pl.BlockSpec(memory_space=pl.ANY)
    count = devices * rows
    return pl.pallas_call(
        functools.partial(fused_kernel, plans, devices),
        in_specs=[pl.BlockSpec(memory_space=pltpu.SMEM), anywhere, anywhere, anywhere],
        out_specs=anywhere,
        out_shape=jax.ShapeDtypeStruct((seqs, rows, width), jnp.bfloat16),
        scratch_shapes=[
            pltpu.VMEM((seqs, layout.key_levels * part, HD), jnp.bfloat16),
            pltpu.VMEM((seqs, layout.key_levels * part, 2 * HD), jnp.bfloat16),
            pltpu.VMEM((seqs, layout.query_levels * part, GROUP * HD), jnp.bfloat16),
            pltpu.VMEM((seqs, layout.query_levels * part, GROUP * HD), jnp.bfloat16),
            pltpu.VMEM((GROUP * rows, 2 * HD), jnp.float32),
            pltpu.VMEM((rows, width), jnp.bfloat16),
            pltpu.SemaphoreType.DMA((seqs, layout.slots, LEVELS)),
            pltpu.SemaphoreType.DMA((per * max(len(layout.sends(z)) for z in range(LEVELS)),)),
            pltpu.SemaphoreType.DMA((most,)),
            pltpu.SemaphoreType.DMA,
        ],
        cost_estimate=pl.CostEstimate(
            flops=4 * seqs * HEADS * count * count * HD // devices,
            bytes_accessed=8 * seqs * rows * width,
            transcendentals=seqs * HEADS * count * count // devices,
        ),
        compiler_params=pltpu.CompilerParams(
            collective_id=collective_id, has_side_effects=True, vmem_limit_bytes=36 * 1024 * 1024
        ),
    )(lengths, *(pltpu.with_memory_space_constraint(x, pltpu.HBM) for x in (queries, keys, values)))


def fused_fits(devices, seqs):
    return devices % LEVELS == 0 and KVH == devices and seqs == len(PLANS)


def attend_block(
    heads,
    width,
    span,
    start,
    valid,
    query_ref,
    at_q,
    key_all,
    value_ext,
    out_ref,
    at_o,
    total_ref,
):
    @pl.when(start >= valid)
    def _():
        out_ref[...] = jnp.zeros_like(out_ref)

    @pl.when(start < valid)
    def _():
        block_q = jnp.concatenate(
            [query_ref[at_q + (slice(None), slice(h * HD, (h + 1) * HD))] for h in range(heads)],
            axis=0,
        )
        total_ref[...] = jnp.zeros_like(total_ref)

        def step(block, masked):
            first = pl.multiple_of(block * span, span)
            held = pl.ds(first, span)
            score = lax.dot_general(
                block_q,
                key_all[held, :],
                (((1,), (1,)), ((), ())),
                preferred_element_type=jnp.float32,
            )
            weight = jnp.exp2(jnp.tanh(score * SCORE_SCALE) * EXP_SCALE)
            if masked:
                shape = (width, span)
                key_pos = first + lax.broadcasted_iota(jnp.int32, shape, 1)
                query_pos = start + lax.broadcasted_iota(jnp.int32, shape, 0)
                allowed = (key_pos <= query_pos) & (key_pos < valid)
                weight = jnp.concatenate(
                    [
                        jnp.where(allowed, weight[h * width : (h + 1) * width], 0.0)
                        for h in range(heads)
                    ],
                    axis=0,
                )
            total_ref[...] += jnp.dot(
                weight.astype(jnp.bfloat16),
                value_ext[held, :],
                preferred_element_type=jnp.float32,
            )

        full = jnp.minimum(start + 1, valid) // span
        stop = (jnp.minimum(start + width, valid) + span - 1) // span

        def plain(block, carry):
            step(block, False)
            return carry

        def edge(block, carry):
            step(block, True)
            return carry

        lax.fori_loop(0, full, plain, 0)
        lax.fori_loop(full, stop, edge, 0)
        live = start + lax.broadcasted_iota(jnp.int32, (width, HD), 0) < valid
        for h in range(heads):
            part = slice(h * width, (h + 1) * width)
            mixed = total_ref[part, :HD] / total_ref[part, HD:]
            out_ref[at_o + (slice(None), slice(h * HD, (h + 1) * HD))] = jnp.where(
                live, mixed, 0.0
            ).astype(jnp.bfloat16)


def attend_kernel(heads, width, span, length_ref, packed_ref, out_ref, key_all, value_ext, total_ref):
    index = pl.program_id(0)
    count = packed_ref.shape[0]
    start = pl.multiple_of(index * width, width)

    @pl.when(index == 0)
    def _():
        key_all[...] = packed_ref[:, heads * HD : (heads + 1) * HD]
        value_ext[:, :HD] = packed_ref[:, (heads + 1) * HD :]
        value_ext[:, HD:] = jnp.ones((count, HD), jnp.bfloat16)

    query = packed_ref.at[pl.ds(start, width)]
    attend_block(
        heads, width, span, start, length_ref[0], query, (), key_all, value_ext, out_ref, (), total_ref
    )


def attend(packed, valid, heads):
    count = packed.shape[0]
    width = min(256, count)
    span = min(512, count)
    return pl.pallas_call(
        functools.partial(attend_kernel, heads, width, span),
        grid_spec=pltpu.PrefetchScalarGridSpec(
            num_scalar_prefetch=1,
            grid=(count // width,),
            in_specs=[pl.BlockSpec((count, (heads + 2) * HD), lambda i, _: (0, 0))],
            out_specs=pl.BlockSpec((width, heads * HD), lambda i, _: (i, 0)),
            scratch_shapes=[
                pltpu.VMEM((count, HD), jnp.bfloat16),
                pltpu.VMEM((count, 2 * HD), jnp.bfloat16),
                pltpu.VMEM((heads * width, 2 * HD), jnp.float32),
            ],
        ),
        out_shape=jax.ShapeDtypeStruct((count, heads * HD), jnp.bfloat16),
        cost_estimate=pl.CostEstimate(
            flops=4 * heads * count * count * HD,
            bytes_accessed=2 * count * HD * (2 * heads + 2),
            transcendentals=heads * count * count,
        ),
        compiler_params=pltpu.CompilerParams(
            dimension_semantics=("arbitrary",), vmem_limit_bytes=40 * 1024 * 1024
        ),
    )(valid, packed)


def exchange(array):
    return lax.all_to_all(
        array, "tp", split_axis=0, concat_axis=0, tiled=True
    )


def per_device(queries, keys, values, lengths):
    seqs, rows, _ = queries.shape
    devices = lax.axis_size("tp")
    count = devices * rows
    if fused_fits(devices, seqs):
        return fused(queries, keys, values, lengths, PLANS, 0)

    pairs = seqs * HEADS
    owned = pairs // devices
    heads_q = queries.reshape(seqs, rows, HEADS, HD)
    heads_k = jnp.repeat(keys.reshape(seqs, rows, KVH, HD), GROUP, axis=2)
    heads_v = jnp.repeat(values.reshape(seqs, rows, KVH, HD), GROUP, axis=2)
    packed = jnp.concatenate([heads_q, heads_k, heads_v], axis=3)
    packed = packed.transpose(0, 2, 1, 3).reshape(devices, owned * rows, 3 * HD)
    gathered = exchange(packed).reshape(devices, owned, rows, 3 * HD)
    outs = []
    for o in range(owned):
        seq = (lax.axis_index("tp") * owned + o) // HEADS
        valid = jnp.sum(jnp.where(jnp.arange(seqs) == seq, lengths, 0))[None]
        outs.append(attend(gathered[:, o].reshape(count, 3 * HD), valid, 1))
    output = jnp.stack(outs).reshape(owned, devices, rows, HD).transpose(1, 0, 2, 3)
    returned = exchange(output.reshape(devices, owned * rows, HD))
    return (
        returned.reshape(seqs, HEADS, rows, HD)
        .transpose(0, 2, 1, 3)
        .reshape(seqs, rows, HEADS * HD)
    )


def solution(mesh):
    placed = (
        P("groups", "tp", None),
        P("groups", "tp", None),
        P("groups", "tp", None),
        P("groups"),
    )
    return jax.shard_map(
        per_device, mesh=mesh, in_specs=placed, out_specs=P("groups", "tp", None), check_vma=False
    )
```

```python
import functools
import math

import jax
import jax.numpy as jnp
from jax import lax
from jax.experimental import pallas as pl
from jax.experimental.pallas import tpu as pltpu
from jax.sharding import PartitionSpec as P

HEADS = 32
KVH = 16
HD = 128
GROUP = HEADS // KVH

SOFT_CAP = 50.0
SCORE_SCALE = 1.0 / (math.sqrt(144.0) * SOFT_CAP)
EXP_SCALE = SOFT_CAP * math.log2(math.e)

LEVELS = 8
PLANS = (
    (
        "030333",
        "012222",
        "002222",
        "013333",
        "004044",
        "011155",
        "000777",
        "010166",
    ),
    (
        "22222222",
        "33333333",
        "00004444",
        "11115555",
        "00004444",
        "11115555",
        "00006666",
        "11117777",
    ),
)
MESH = pl.DeviceIdType.MESH


class Layout:
    def __init__(self, plans):
        self.owner = [[[int(z) for z in row] for row in plan] for plan in plans]
        self.key_at, self.query_at, self.slot = {}, {}, {}
        self.items = [[] for _ in range(LEVELS)]
        self.key_levels = self.query_levels = self.slots = 0
        for level in range(LEVELS):
            for s, plan in enumerate(self.owner):
                keys = queries = slots = 0
                for k, row in enumerate(plan):
                    asked = [z for z, owner in enumerate(row) if owner == level]
                    if not asked:
                        continue
                    self.key_at[s, k, level] = keys
                    self.slot[s, k, level] = slots
                    seen = 0
                    for z in asked:
                        self.query_at[s, k, z] = queries
                        self.items[level].append((s, k, z, slots, keys, queries, seen, asked))
                        queries += 1
                        seen = z + 1
                    keys += asked[-1] + 1
                    slots += 1
                self.key_levels = max(self.key_levels, keys)
                self.query_levels = max(self.query_levels, queries)
                self.slots = max(self.slots, slots)

    @staticmethod
    def way(level, to):
        return (to // 2 > level // 2) - (to // 2 < level // 2), (to ^ level) & 1

    def sends(self, level):
        listed = []
        for s, plan in enumerate(self.owner):
            for k, row in enumerate(plan):
                if level >= len(row):
                    continue
                for to in sorted(set(row[level:])):
                    query = 1 + self.query_at[s, k, level] if to == row[level] else 0
                    listed.append((s, k, to, query, self.slot[s, k, to], self.key_at[s, k, to]))

        def rank(sent):
            s, k, to, query, _, _ = sent
            return (s, k // 2)

        ordered = []
        for group in sorted({rank(sent) for sent in listed}):
            buckets = {}
            for sent in listed:
                if rank(sent) == group:
                    buckets.setdefault(self.way(level, sent[2]), []).append(sent)
            spaced = []
            for way, bucket in sorted(buckets.items()):
                bucket.sort(key=lambda x: x[3] > 0)
                spaced += [((n + 0.5) / len(bucket), way, x) for n, x in enumerate(bucket)]
            ordered += [x for _, _, x in sorted(spaced)]
        return ordered

    def active(self, s):
        return len(self.owner[s][0])


def pick(values, index):
    if all(isinstance(v, int) and v == values[0] for v in values):
        return values[0]
    result = jnp.int32(values[-1])
    for n in reversed(range(len(values) - 1)):
        result = jnp.where(index == n, values[n], result)
    return result


def columns_of(items, code, level):
    most = max(len(listed) for listed in items)
    codes = [[code(item) for item in listed] or [0] for listed in items]
    return [pick([row[min(n, len(row) - 1)] for row in codes], level) for n in range(most)]


def pack_fields(fields, bits):
    return sum(field << (bits * n) for n, field in enumerate(fields))


def split_fields(code, bits, count):
    return [(code >> (bits * n)) & ((1 << bits) - 1) for n in range(count)]


def fused_kernel(
    plans,
    devices,
    length_ref,
    query_ref,
    key_ref,
    value_ref,
    out_ref,
    key_all,
    value_ext,
    query_all,
    mixed_all,
    total_ref,
    blank,
    arrived,
    sent_in,
    sent_out,
    returned,
):
    layout = Layout(plans)
    seqs = len(plans)
    per = devices // LEVELS
    rows = query_ref.shape[1]
    part = per * rows
    span = min(512, part)
    size = GROUP * HD
    me = lax.axis_index("tp")
    level, lane = me // per, me % per

    barrier = pltpu.get_barrier_semaphore()
    for d in range(1, devices):
        pl.semaphore_signal(
            barrier, inc=1, device_id={"tp": lax.rem(me + d, devices)}, device_id_type=MESH
        )
    pl.semaphore_wait(barrier, devices - 1)

    def send(source, target, sent, landed, to):
        @pl.when(to == me)
        def _():
            pltpu.make_async_copy(source, target, landed).start()

        @pl.when(to != me)
        def _():
            pltpu.make_async_remote_copy(
                src_ref=source,
                dst_ref=target,
                send_sem=sent,
                recv_sem=landed,
                device_id={"tp": to},
                device_id_type=MESH,
            ).start()

    def tile(x, width):
        return pl.ds(pl.multiple_of(x * width, width), width)

    def wait(ref, sem):
        pltpu.make_async_copy(ref, ref, sem).wait()

    sends = [layout.sends(z) for z in range(LEVELS)]
    groups = pick([len(listed) for listed in sends], level) * per

    send_codes = columns_of(sends, lambda i: pack_fields((i[0], i[1], i[2], i[4]), 6), level)
    send_rows = columns_of(sends, lambda i: pack_fields((i[3], i[5]), 6), level)

    def send_info(index):
        n, step = index // per, index % per
        n = jnp.where((n ^ (lane & 1)) * per < groups, n ^ (lane & 1), n)
        s, k, to, slot = split_fields(pick(send_codes, n), 6, 4)
        query, key_at = split_fields(pick(send_rows, n), 6, 2)
        other = lax.rem(lane + step, per)
        return s, k * per + other, to * per + other, query, slot, key_at

    def spread(index, carry):
        s, head, dest, query, slot, key_at = send_info(index)
        landed, sent = arrived.at[s, slot, level], sent_in.at[index]
        target = tile(key_at * per + me, rows)

        @pl.when(query > 0)
        def _():
            target_q = tile((query - 1) * per + lane, rows)
            send(
                query_ref.at[s, :, tile(head, size)],
                query_all.at[s, target_q],
                sent,
                landed,
                dest,
            )

        send(key_ref.at[s, :, tile(head, HD)], key_all.at[s, target], sent, landed, dest)
        send(
            value_ref.at[s, :, tile(head, HD)],
            value_ext.at[s, target, pl.ds(0, HD)],
            sent,
            landed,
            dest,
        )
        return carry

    lax.fori_loop(0, groups, spread, 0)

    idle = [s for s in range(seqs) if layout.active(s) < LEVELS]
    if idle:
        blank[...] = jnp.zeros_like(blank)
        for s in idle:

            @pl.when(level >= layout.active(s))
            def _(s=s):
                pltpu.make_async_copy(blank, out_ref.at[s], returned).start()

    blocks = pick([len(listed) * per for listed in layout.items], level)

    item_codes = columns_of(layout.items, lambda i: pack_fields(i[:5], 6), level)
    item_rows = columns_of(
        layout.items,
        lambda i: pack_fields((i[5], i[6]), 6) + (sum(1 << z for z in i[7]) << 12),
        level,
    )

    def block_info(index):
        item, j = index // per, index % per
        code, more = pick(item_codes, item), pick(item_rows, item)
        return *split_fields(code, 6, 5), *split_fields(more, 6, 2), more >> 12, j

    def return_block(index):
        s, k, z, _, _, query_at, _, _, j = block_info(index)
        send(
            mixed_all.at[s, tile(query_at * per + j, rows)],
            out_ref.at[s, :, tile(k * per + lane, size)],
            sent_out.at[index],
            returned,
            z * per + j,
        )

    def attend(index, carry):
        s, k, z, slot, key_at, query_at, seen, asked, j = block_info(index)
        valid = length_ref[s]
        key_base = key_at * part

        @pl.when(j == 0)
        def _():
            def take(source, carry):
                asks = (asked >> source) & 1

                @pl.when(asks == 1)
                def _():
                    wait(query_all.at[0, pl.ds(0, 2 * part)], arrived.at[s, slot, source])

                @pl.when(asks == 0)
                def _():
                    wait(query_all.at[0, pl.ds(0, part)], arrived.at[s, slot, source])

                def extend(n, carry):
                    first = pl.multiple_of(source * part + n * rows, rows)
                    held = pl.ds(pl.multiple_of(key_base + first, rows), rows)
                    pos = first + lax.broadcasted_iota(jnp.int32, (rows, 2 * HD), 0)
                    block = value_ext[s, held, :HD].astype(jnp.float32)
                    block = jnp.concatenate([block, jnp.ones_like(block)], axis=1)
                    value_ext[s, held, :] = jnp.where(pos < valid, block, 0.0).astype(jnp.bfloat16)
                    return carry

                lax.fori_loop(0, per, extend, 0)
                return carry

            lax.fori_loop(seen, z + 1, take, 0)

        start = (z * per + j) * rows
        held_q = tile(query_at * per + j, rows)
        block_q = jnp.concatenate(
            [query_all[s, held_q, h * HD : (h + 1) * HD] for h in range(GROUP)], axis=0
        )
        total_ref[...] = jnp.zeros_like(total_ref)

        def step(block, masked):
            first = pl.multiple_of(block * span, span)
            held = pl.ds(pl.multiple_of(key_base + first, span), span)
            score = lax.dot_general(
                block_q,
                key_all[s, held, :],
                (((1,), (1,)), ((), ())),
                preferred_element_type=jnp.float32,
            )
            weight = jnp.exp2(jnp.tanh(score * SCORE_SCALE) * EXP_SCALE)
            if masked:
                shape = (rows, span)
                allowed = first + lax.broadcasted_iota(
                    jnp.int32, shape, 1
                ) <= start + lax.broadcasted_iota(jnp.int32, shape, 0)
                weight = jnp.concatenate(
                    [
                        jnp.where(allowed, weight[h * rows : (h + 1) * rows], 0.0)
                        for h in range(GROUP)
                    ],
                    axis=0,
                )
            total_ref[...] += jnp.dot(
                weight.astype(jnp.bfloat16),
                value_ext[s, held, :],
                preferred_element_type=jnp.float32,
            )

        def plain(block, carry):
            step(block, False)
            return carry

        full = start // span
        lax.fori_loop(0, full, plain, 0)
        step(full, True)

        live = start + lax.broadcasted_iota(jnp.int32, (rows, HD), 0) < valid
        for h in range(GROUP):
            at = slice(h * rows, (h + 1) * rows)
            mixed = total_ref[at, :HD] / total_ref[at, HD:]
            mixed_all[s, held_q, h * HD : (h + 1) * HD] = jnp.where(live, mixed, 0.0).astype(
                jnp.bfloat16
            )

        @pl.when(index > 0)
        def _():
            return_block(index - 1)

        return carry

    lax.fori_loop(0, blocks, attend, 0)

    def settle(index, carry):
        _, _, dest, query, _, _ = send_info(index)

        @pl.when((dest != me) & (query > 0))
        def _():
            wait(query_all.at[0, pl.ds(0, 2 * rows)], sent_in.at[index])

        @pl.when((dest != me) & (query == 0))
        def _():
            wait(query_all.at[0, pl.ds(0, rows)], sent_in.at[index])

        return carry

    lax.fori_loop(0, groups, settle, 0)

    @pl.when(blocks > 0)
    def _():
        return_block(blocks - 1)

    def settle_out(index, carry):
        _, _, z, _, _, _, _, _, j = block_info(index)

        @pl.when(z * per + j != me)
        def _():
            wait(mixed_all.at[0, pl.ds(0, rows)], sent_out.at[index])

        return carry

    lax.fori_loop(0, blocks, settle_out, 0)
    wait(out_ref, returned)


def fused(queries, keys, values, lengths, plans, collective_id):
    seqs, rows, width = queries.shape
    devices = lax.axis_size("tp")
    per = devices // LEVELS
    part = per * rows
    layout = Layout(plans)
    most = per * max(len(listed) for listed in layout.items)
    anywhere = pl.BlockSpec(memory_space=pl.ANY)
    count = devices * rows
    held = seqs * part * HD * (3 * layout.key_levels + 2 * GROUP * layout.query_levels)
    limit = 2 * (held + rows * width) + 8 * GROUP * rows * HD + 8 * 1024 * 1024
    pinned = [pltpu.with_memory_space_constraint(x, pltpu.HBM) for x in (queries, keys, values)]
    return pl.pallas_call(
        functools.partial(fused_kernel, plans, devices),
        in_specs=[pl.BlockSpec(memory_space=pltpu.SMEM), anywhere, anywhere, anywhere],
        out_specs=anywhere,
        out_shape=jax.ShapeDtypeStruct((seqs, rows, width), jnp.bfloat16),
        scratch_shapes=[
            pltpu.VMEM((seqs, layout.key_levels * part, HD), jnp.bfloat16),
            pltpu.VMEM((seqs, layout.key_levels * part, 2 * HD), jnp.bfloat16),
            pltpu.VMEM((seqs, layout.query_levels * part, GROUP * HD), jnp.bfloat16),
            pltpu.VMEM((seqs, layout.query_levels * part, GROUP * HD), jnp.bfloat16),
            pltpu.VMEM((GROUP * rows, 2 * HD), jnp.float32),
            pltpu.VMEM((rows, width), jnp.bfloat16),
            pltpu.SemaphoreType.DMA((seqs, layout.slots, LEVELS)),
            pltpu.SemaphoreType.DMA((per * max(len(layout.sends(z)) for z in range(LEVELS)),)),
            pltpu.SemaphoreType.DMA((most,)),
            pltpu.SemaphoreType.DMA,
        ],
        cost_estimate=pl.CostEstimate(
            flops=4 * seqs * HEADS * count * count * HD // devices,
            bytes_accessed=8 * seqs * rows * width,
            transcendentals=seqs * HEADS * count * count // devices,
        ),
        compiler_params=pltpu.CompilerParams(
            collective_id=collective_id, has_side_effects=True, vmem_limit_bytes=limit
        ),
    )(lengths, *pinned)


def fused_fits(devices):
    return devices % LEVELS == 0 and KVH == devices


def fused_by_length(queries, keys, values, lengths):
    seqs, rows, _ = queries.shape
    part = lax.axis_size("tp") // LEVELS * rows
    longest = lax.pmax(lengths, "groups")
    index, choices = 0, [()]
    for s in range(seqs):
        need = sum((longest[s] > len(plan[0]) * part).astype(jnp.int32) for plan in PLANS[:-1])
        index = index * len(PLANS) + need
        choices = [plans + (plan,) for plans in choices for plan in PLANS]
    branches = [
        functools.partial(fused, plans=plans, collective_id=n) for n, plans in enumerate(choices)
    ]
    return lax.switch(index, branches, queries, keys, values, lengths)


def attend_block(
    heads,
    width,
    span,
    start,
    valid,
    query_ref,
    at_q,
    key_all,
    value_ext,
    out_ref,
    at_o,
    total_ref,
):
    @pl.when(start >= valid)
    def _():
        out_ref[...] = jnp.zeros_like(out_ref)

    @pl.when(start < valid)
    def _():
        block_q = jnp.concatenate(
            [query_ref[at_q + (slice(None), slice(h * HD, (h + 1) * HD))] for h in range(heads)],
            axis=0,
        )
        total_ref[...] = jnp.zeros_like(total_ref)

        def step(block, masked):
            first = pl.multiple_of(block * span, span)
            held = pl.ds(first, span)
            score = lax.dot_general(
                block_q,
                key_all[held, :],
                (((1,), (1,)), ((), ())),
                preferred_element_type=jnp.float32,
            )
            weight = jnp.exp2(jnp.tanh(score * SCORE_SCALE) * EXP_SCALE)
            if masked:
                shape = (width, span)
                key_pos = first + lax.broadcasted_iota(jnp.int32, shape, 1)
                query_pos = start + lax.broadcasted_iota(jnp.int32, shape, 0)
                allowed = (key_pos <= query_pos) & (key_pos < valid)
                weight = jnp.concatenate(
                    [
                        jnp.where(allowed, weight[h * width : (h + 1) * width], 0.0)
                        for h in range(heads)
                    ],
                    axis=0,
                )
            total_ref[...] += jnp.dot(
                weight.astype(jnp.bfloat16),
                value_ext[held, :],
                preferred_element_type=jnp.float32,
            )

        full = jnp.minimum(start + 1, valid) // span
        stop = (jnp.minimum(start + width, valid) + span - 1) // span

        def plain(block, carry):
            step(block, False)
            return carry

        def edge(block, carry):
            step(block, True)
            return carry

        lax.fori_loop(0, full, plain, 0)
        lax.fori_loop(full, stop, edge, 0)
        live = start + lax.broadcasted_iota(jnp.int32, (width, HD), 0) < valid
        for h in range(heads):
            part = slice(h * width, (h + 1) * width)
            mixed = total_ref[part, :HD] / total_ref[part, HD:]
            out_ref[at_o + (slice(None), slice(h * HD, (h + 1) * HD))] = jnp.where(
                live, mixed, 0.0
            ).astype(jnp.bfloat16)


def attend_kernel(heads, width, span, length_ref, packed_ref, out_ref, key_all, value_ext, total_ref):
    index = pl.program_id(0)
    count = packed_ref.shape[0]
    start = pl.multiple_of(index * width, width)

    @pl.when(index == 0)
    def _():
        key_all[...] = packed_ref[:, heads * HD : (heads + 1) * HD]
        value_ext[:, :HD] = packed_ref[:, (heads + 1) * HD :]
        value_ext[:, HD:] = jnp.ones((count, HD), jnp.bfloat16)

    query = packed_ref.at[pl.ds(start, width)]
    attend_block(
        heads, width, span, start, length_ref[0], query, (), key_all, value_ext, out_ref, (), total_ref
    )


def attend(packed, valid, heads):
    count = packed.shape[0]
    width = min(256, count)
    span = min(512, count)
    return pl.pallas_call(
        functools.partial(attend_kernel, heads, width, span),
        grid_spec=pltpu.PrefetchScalarGridSpec(
            num_scalar_prefetch=1,
            grid=(count // width,),
            in_specs=[pl.BlockSpec((count, (heads + 2) * HD), lambda i, _: (0, 0))],
            out_specs=pl.BlockSpec((width, heads * HD), lambda i, _: (i, 0)),
            scratch_shapes=[
                pltpu.VMEM((count, HD), jnp.bfloat16),
                pltpu.VMEM((count, 2 * HD), jnp.bfloat16),
                pltpu.VMEM((heads * width, 2 * HD), jnp.float32),
            ],
        ),
        out_shape=jax.ShapeDtypeStruct((count, heads * HD), jnp.bfloat16),
        cost_estimate=pl.CostEstimate(
            flops=4 * heads * count * count * HD,
            bytes_accessed=2 * count * HD * (2 * heads + 2),
            transcendentals=heads * count * count,
        ),
        compiler_params=pltpu.CompilerParams(
            dimension_semantics=("arbitrary",), vmem_limit_bytes=40 * 1024 * 1024
        ),
    )(valid, packed)


def exchange(array):
    return lax.all_to_all(
        array, "tp", split_axis=0, concat_axis=0, tiled=True
    )


def per_device(queries, keys, values, lengths):
    seqs, rows, _ = queries.shape
    devices = lax.axis_size("tp")
    count = devices * rows
    if fused_fits(devices):
        return fused_by_length(queries, keys, values, lengths)

    pairs = seqs * HEADS
    owned = pairs // devices
    heads_q = queries.reshape(seqs, rows, HEADS, HD)
    heads_k = jnp.repeat(keys.reshape(seqs, rows, KVH, HD), GROUP, axis=2)
    heads_v = jnp.repeat(values.reshape(seqs, rows, KVH, HD), GROUP, axis=2)
    packed = jnp.concatenate([heads_q, heads_k, heads_v], axis=3)
    packed = packed.transpose(0, 2, 1, 3).reshape(devices, owned * rows, 3 * HD)
    gathered = exchange(packed).reshape(devices, owned, rows, 3 * HD)
    outs = []
    for o in range(owned):
        seq = (lax.axis_index("tp") * owned + o) // HEADS
        valid = jnp.sum(jnp.where(jnp.arange(seqs) == seq, lengths, 0))[None]
        outs.append(attend(gathered[:, o].reshape(count, 3 * HD), valid, 1))
    output = jnp.stack(outs).reshape(owned, devices, rows, HD).transpose(1, 0, 2, 3)
    returned = exchange(output.reshape(devices, owned * rows, HD))
    return (
        returned.reshape(seqs, HEADS, rows, HD)
        .transpose(0, 2, 1, 3)
        .reshape(seqs, rows, HEADS * HD)
    )


def solution(mesh):
    placed = (
        P("groups", "tp", None),
        P("groups", "tp", None),
        P("groups", "tp", None),
        P("groups"),
    )
    return jax.shard_map(
        per_device, mesh=mesh, in_specs=placed, out_specs=P("groups", "tp", None), check_vma=False
    )
```

```python
import functools
import math

import jax
import jax.numpy as jnp
from jax import lax
from jax.experimental import pallas as pl
from jax.experimental.pallas import tpu as pltpu
from jax.sharding import PartitionSpec as P

HEADS = 32
KVH = 16
HD = 128
GROUP = HEADS // KVH

SOFT_CAP = 50.0
SCORE_SCALE = 1.0 / (math.sqrt(144.0) * SOFT_CAP)
EXP_SCALE = SOFT_CAP * math.log2(math.e)

LEVELS = 8
PLANS = (
    (
        "00222",
        "01333",
        "01212",
        "00330",
        "00222",
        "01414",
        "01014",
        "00055",
    ),
    (
        "030333",
        "012222",
        "002222",
        "013333",
        "004044",
        "011155",
        "000777",
        "010166",
    ),
    (
        "22222222",
        "33333333",
        "00004444",
        "11115555",
        "00004444",
        "11115555",
        "00006666",
        "11117777",
    ),
)
MESH = pl.DeviceIdType.MESH


class Layout:
    def __init__(self, plans):
        self.owner = [[[int(z) for z in row] for row in plan] for plan in plans]
        self.key_at, self.query_at, self.slot = {}, {}, {}
        self.items = [[] for _ in range(LEVELS)]
        self.key_levels = self.query_levels = self.slots = 0
        for level in range(LEVELS):
            for s, plan in enumerate(self.owner):
                keys = queries = slots = 0
                for k, row in enumerate(plan):
                    asked = [z for z, owner in enumerate(row) if owner == level]
                    if not asked:
                        continue
                    self.key_at[s, k, level] = keys
                    self.slot[s, k, level] = slots
                    seen = 0
                    for z in asked:
                        self.query_at[s, k, z] = queries
                        self.items[level].append((s, k, z, slots, keys, queries, seen, asked))
                        queries += 1
                        seen = z + 1
                    keys += asked[-1] + 1
                    slots += 1
                self.key_levels = max(self.key_levels, keys)
                self.query_levels = max(self.query_levels, queries)
                self.slots = max(self.slots, slots)

    @staticmethod
    def way(level, to):
        return (to // 2 > level // 2) - (to // 2 < level // 2), (to ^ level) & 1

    def sends(self, level):
        listed = []
        for s, plan in enumerate(self.owner):
            for k, row in enumerate(plan):
                if level >= len(row):
                    continue
                for to in sorted(set(row[level:])):
                    query = 1 + self.query_at[s, k, level] if to == row[level] else 0
                    listed.append((s, k, to, query, self.slot[s, k, to], self.key_at[s, k, to]))

        def rank(sent):
            s, k, to, query, _, _ = sent
            return (s, k // 2)

        ordered = []
        for group in sorted({rank(sent) for sent in listed}):
            buckets = {}
            for sent in listed:
                if rank(sent) == group:
                    buckets.setdefault(self.way(level, sent[2]), []).append(sent)
            spaced = []
            for way, bucket in sorted(buckets.items()):
                bucket.sort(key=lambda x: x[3] > 0)
                spaced += [((n + 0.5) / len(bucket), way, x) for n, x in enumerate(bucket)]
            ordered += [x for _, _, x in sorted(spaced)]
        return ordered

    def active(self, s):
        return len(self.owner[s][0])


def pick(values, index):
    if all(isinstance(v, int) and v == values[0] for v in values):
        return values[0]
    result = jnp.int32(values[-1])
    for n in reversed(range(len(values) - 1)):
        result = jnp.where(index == n, values[n], result)
    return result


def columns_of(items, code, level):
    most = max(len(listed) for listed in items)
    codes = [[code(item) for item in listed] or [0] for listed in items]
    return [pick([row[min(n, len(row) - 1)] for row in codes], level) for n in range(most)]


def pack_fields(fields, bits):
    return sum(field << (bits * n) for n, field in enumerate(fields))


def split_fields(code, bits, count):
    return [(code >> (bits * n)) & ((1 << bits) - 1) for n in range(count)]


def fused_kernel(
    plans,
    devices,
    length_ref,
    query_ref,
    key_ref,
    value_ref,
    out_ref,
    key_all,
    value_ext,
    query_all,
    mixed_all,
    total_ref,
    blank,
    arrived,
    sent_in,
    sent_out,
    returned,
):
    layout = Layout(plans)
    seqs = len(plans)
    per = devices // LEVELS
    rows = query_ref.shape[1]
    part = per * rows
    span = min(512, part)
    size = GROUP * HD
    me = lax.axis_index("tp")
    level, lane = me // per, me % per

    barrier = pltpu.get_barrier_semaphore()
    for d in range(1, devices):
        pl.semaphore_signal(
            barrier, inc=1, device_id={"tp": lax.rem(me + d, devices)}, device_id_type=MESH
        )
    pl.semaphore_wait(barrier, devices - 1)

    def send(source, target, sent, landed, to):
        @pl.when(to == me)
        def _():
            pltpu.make_async_copy(source, target, landed).start()

        @pl.when(to != me)
        def _():
            pltpu.make_async_remote_copy(
                src_ref=source,
                dst_ref=target,
                send_sem=sent,
                recv_sem=landed,
                device_id={"tp": to},
                device_id_type=MESH,
            ).start()

    def tile(x, width):
        return pl.ds(pl.multiple_of(x * width, width), width)

    def wait(ref, sem):
        pltpu.make_async_copy(ref, ref, sem).wait()

    sends = [layout.sends(z) for z in range(LEVELS)]
    groups = pick([len(listed) for listed in sends], level) * per

    send_codes = columns_of(sends, lambda i: pack_fields((i[0], i[1], i[2], i[4]), 6), level)
    send_rows = columns_of(sends, lambda i: pack_fields((i[3], i[5]), 6), level)

    def send_info(index):
        n, step = index // per, index % per
        n = jnp.where((n ^ (lane & 1)) * per < groups, n ^ (lane & 1), n)
        s, k, to, slot = split_fields(pick(send_codes, n), 6, 4)
        query, key_at = split_fields(pick(send_rows, n), 6, 2)
        other = lax.rem(lane + step, per)
        return s, k * per + other, to * per + other, query, slot, key_at

    def spread(index, carry):
        s, head, dest, query, slot, key_at = send_info(index)
        landed, sent = arrived.at[s, slot, level], sent_in.at[index]
        target = tile(key_at * per + me, rows)

        @pl.when(query > 0)
        def _():
            target_q = tile((query - 1) * per + lane, rows)
            send(
                query_ref.at[s, :, tile(head, size)],
                query_all.at[s, target_q],
                sent,
                landed,
                dest,
            )

        send(key_ref.at[s, :, tile(head, HD)], key_all.at[s, target], sent, landed, dest)
        send(
            value_ref.at[s, :, tile(head, HD)],
            value_ext.at[s, target, pl.ds(0, HD)],
            sent,
            landed,
            dest,
        )
        return carry

    lax.fori_loop(0, groups, spread, 0)

    idle = [s for s in range(seqs) if layout.active(s) < LEVELS]
    if idle:
        blank[...] = jnp.zeros_like(blank)
        for s in idle:

            @pl.when(level >= layout.active(s))
            def _(s=s):
                pltpu.make_async_copy(blank, out_ref.at[s], returned).start()

    blocks = pick([len(listed) * per for listed in layout.items], level)

    item_codes = columns_of(layout.items, lambda i: pack_fields(i[:5], 6), level)
    item_rows = columns_of(
        layout.items,
        lambda i: pack_fields((i[5], i[6]), 6) + (sum(1 << z for z in i[7]) << 12),
        level,
    )

    def block_info(index):
        item, j = index // per, index % per
        code, more = pick(item_codes, item), pick(item_rows, item)
        return *split_fields(code, 6, 5), *split_fields(more, 6, 2), more >> 12, j

    def return_block(index):
        s, k, z, _, _, query_at, _, _, j = block_info(index)
        send(
            mixed_all.at[s, tile(query_at * per + j, rows)],
            out_ref.at[s, :, tile(k * per + lane, size)],
            sent_out.at[index],
            returned,
            z * per + j,
        )

    def attend(index, carry):
        s, k, z, slot, key_at, query_at, seen, asked, j = block_info(index)
        valid = length_ref[s]
        key_base = key_at * part

        @pl.when(j == 0)
        def _():
            def take(source, carry):
                asks = (asked >> source) & 1

                @pl.when(asks == 1)
                def _():
                    wait(query_all.at[0, pl.ds(0, 2 * part)], arrived.at[s, slot, source])

                @pl.when(asks == 0)
                def _():
                    wait(query_all.at[0, pl.ds(0, part)], arrived.at[s, slot, source])

                def extend(n, carry):
                    first = pl.multiple_of(source * part + n * rows, rows)
                    held = pl.ds(pl.multiple_of(key_base + first, rows), rows)
                    pos = first + lax.broadcasted_iota(jnp.int32, (rows, 2 * HD), 0)
                    block = value_ext[s, held, :HD].astype(jnp.float32)
                    block = jnp.concatenate([block, jnp.ones_like(block)], axis=1)
                    value_ext[s, held, :] = jnp.where(pos < valid, block, 0.0).astype(jnp.bfloat16)
                    return carry

                lax.fori_loop(0, per, extend, 0)
                return carry

            lax.fori_loop(seen, z + 1, take, 0)

        start = (z * per + j) * rows
        held_q = tile(query_at * per + j, rows)
        block_q = jnp.concatenate(
            [query_all[s, held_q, h * HD : (h + 1) * HD] for h in range(GROUP)], axis=0
        )
        total_ref[...] = jnp.zeros_like(total_ref)

        def step(block, masked):
            first = pl.multiple_of(block * span, span)
            held = pl.ds(pl.multiple_of(key_base + first, span), span)
            score = lax.dot_general(
                block_q,
                key_all[s, held, :],
                (((1,), (1,)), ((), ())),
                preferred_element_type=jnp.float32,
            )
            weight = jnp.exp2(jnp.tanh(score * SCORE_SCALE) * EXP_SCALE)
            if masked:
                shape = (rows, span)
                allowed = first + lax.broadcasted_iota(
                    jnp.int32, shape, 1
                ) <= start + lax.broadcasted_iota(jnp.int32, shape, 0)
                weight = jnp.concatenate(
                    [
                        jnp.where(allowed, weight[h * rows : (h + 1) * rows], 0.0)
                        for h in range(GROUP)
                    ],
                    axis=0,
                )
            total_ref[...] += jnp.dot(
                weight.astype(jnp.bfloat16),
                value_ext[s, held, :],
                preferred_element_type=jnp.float32,
            )

        def plain(block, carry):
            step(block, False)
            return carry

        full = start // span
        lax.fori_loop(0, full, plain, 0)
        step(full, True)

        live = start + lax.broadcasted_iota(jnp.int32, (rows, HD), 0) < valid
        for h in range(GROUP):
            at = slice(h * rows, (h + 1) * rows)
            mixed = total_ref[at, :HD] / total_ref[at, HD:]
            mixed_all[s, held_q, h * HD : (h + 1) * HD] = jnp.where(live, mixed, 0.0).astype(
                jnp.bfloat16
            )

        @pl.when(index > 0)
        def _():
            return_block(index - 1)

        return carry

    lax.fori_loop(0, blocks, attend, 0)

    def settle(index, carry):
        _, _, dest, query, _, _ = send_info(index)

        @pl.when((dest != me) & (query > 0))
        def _():
            wait(query_all.at[0, pl.ds(0, 2 * rows)], sent_in.at[index])

        @pl.when((dest != me) & (query == 0))
        def _():
            wait(query_all.at[0, pl.ds(0, rows)], sent_in.at[index])

        return carry

    lax.fori_loop(0, groups, settle, 0)

    @pl.when(blocks > 0)
    def _():
        return_block(blocks - 1)

    def settle_out(index, carry):
        _, _, z, _, _, _, _, _, j = block_info(index)

        @pl.when(z * per + j != me)
        def _():
            wait(mixed_all.at[0, pl.ds(0, rows)], sent_out.at[index])

        return carry

    lax.fori_loop(0, blocks, settle_out, 0)
    wait(out_ref, returned)


def fused(queries, keys, values, lengths, plans, collective_id):
    seqs, rows, width = queries.shape
    devices = lax.axis_size("tp")
    per = devices // LEVELS
    part = per * rows
    layout = Layout(plans)
    most = per * max(len(listed) for listed in layout.items)
    anywhere = pl.BlockSpec(memory_space=pl.ANY)
    count = devices * rows
    held = seqs * part * HD * (3 * layout.key_levels + 2 * GROUP * layout.query_levels)
    limit = 2 * (held + rows * width) + 8 * GROUP * rows * HD + 8 * 1024 * 1024
    pinned = [pltpu.with_memory_space_constraint(x, pltpu.HBM) for x in (queries, keys, values)]
    return pl.pallas_call(
        functools.partial(fused_kernel, plans, devices),
        in_specs=[pl.BlockSpec(memory_space=pltpu.SMEM), anywhere, anywhere, anywhere],
        out_specs=anywhere,
        out_shape=jax.ShapeDtypeStruct((seqs, rows, width), jnp.bfloat16),
        scratch_shapes=[
            pltpu.VMEM((seqs, layout.key_levels * part, HD), jnp.bfloat16),
            pltpu.VMEM((seqs, layout.key_levels * part, 2 * HD), jnp.bfloat16),
            pltpu.VMEM((seqs, layout.query_levels * part, GROUP * HD), jnp.bfloat16),
            pltpu.VMEM((seqs, layout.query_levels * part, GROUP * HD), jnp.bfloat16),
            pltpu.VMEM((GROUP * rows, 2 * HD), jnp.float32),
            pltpu.VMEM((rows, width), jnp.bfloat16),
            pltpu.SemaphoreType.DMA((seqs, layout.slots, LEVELS)),
            pltpu.SemaphoreType.DMA((per * max(len(layout.sends(z)) for z in range(LEVELS)),)),
            pltpu.SemaphoreType.DMA((most,)),
            pltpu.SemaphoreType.DMA,
        ],
        cost_estimate=pl.CostEstimate(
            flops=4 * seqs * HEADS * count * count * HD // devices,
            bytes_accessed=8 * seqs * rows * width,
            transcendentals=seqs * HEADS * count * count // devices,
        ),
        compiler_params=pltpu.CompilerParams(
            collective_id=collective_id, has_side_effects=True, vmem_limit_bytes=limit
        ),
    )(lengths, *pinned)


def fused_fits(devices):
    return devices % LEVELS == 0 and KVH == devices


def fused_by_length(queries, keys, values, lengths):
    seqs, rows, _ = queries.shape
    part = lax.axis_size("tp") // LEVELS * rows
    longest = lax.pmax(lengths, "groups")
    index, choices = 0, [()]
    for s in range(seqs):
        need = sum((longest[s] > len(plan[0]) * part).astype(jnp.int32) for plan in PLANS[:-1])
        index = index * len(PLANS) + need
        choices = [plans + (plan,) for plans in choices for plan in PLANS]
    branches = [
        functools.partial(fused, plans=plans, collective_id=n) for n, plans in enumerate(choices)
    ]
    return lax.switch(index, branches, queries, keys, values, lengths)


def attend_block(
    heads,
    width,
    span,
    start,
    valid,
    query_ref,
    at_q,
    key_all,
    value_ext,
    out_ref,
    at_o,
    total_ref,
):
    @pl.when(start >= valid)
    def _():
        out_ref[...] = jnp.zeros_like(out_ref)

    @pl.when(start < valid)
    def _():
        block_q = jnp.concatenate(
            [query_ref[at_q + (slice(None), slice(h * HD, (h + 1) * HD))] for h in range(heads)],
            axis=0,
        )
        total_ref[...] = jnp.zeros_like(total_ref)

        def step(block, masked):
            first = pl.multiple_of(block * span, span)
            held = pl.ds(first, span)
            score = lax.dot_general(
                block_q,
                key_all[held, :],
                (((1,), (1,)), ((), ())),
                preferred_element_type=jnp.float32,
            )
            weight = jnp.exp2(jnp.tanh(score * SCORE_SCALE) * EXP_SCALE)
            if masked:
                shape = (width, span)
                key_pos = first + lax.broadcasted_iota(jnp.int32, shape, 1)
                query_pos = start + lax.broadcasted_iota(jnp.int32, shape, 0)
                allowed = (key_pos <= query_pos) & (key_pos < valid)
                weight = jnp.concatenate(
                    [
                        jnp.where(allowed, weight[h * width : (h + 1) * width], 0.0)
                        for h in range(heads)
                    ],
                    axis=0,
                )
            total_ref[...] += jnp.dot(
                weight.astype(jnp.bfloat16),
                value_ext[held, :],
                preferred_element_type=jnp.float32,
            )

        full = jnp.minimum(start + 1, valid) // span
        stop = (jnp.minimum(start + width, valid) + span - 1) // span

        def plain(block, carry):
            step(block, False)
            return carry

        def edge(block, carry):
            step(block, True)
            return carry

        lax.fori_loop(0, full, plain, 0)
        lax.fori_loop(full, stop, edge, 0)
        live = start + lax.broadcasted_iota(jnp.int32, (width, HD), 0) < valid
        for h in range(heads):
            part = slice(h * width, (h + 1) * width)
            mixed = total_ref[part, :HD] / total_ref[part, HD:]
            out_ref[at_o + (slice(None), slice(h * HD, (h + 1) * HD))] = jnp.where(
                live, mixed, 0.0
            ).astype(jnp.bfloat16)


def attend_kernel(heads, width, span, length_ref, packed_ref, out_ref, key_all, value_ext, total_ref):
    index = pl.program_id(0)
    count = packed_ref.shape[0]
    start = pl.multiple_of(index * width, width)

    @pl.when(index == 0)
    def _():
        key_all[...] = packed_ref[:, heads * HD : (heads + 1) * HD]
        value_ext[:, :HD] = packed_ref[:, (heads + 1) * HD :]
        value_ext[:, HD:] = jnp.ones((count, HD), jnp.bfloat16)

    query = packed_ref.at[pl.ds(start, width)]
    attend_block(
        heads, width, span, start, length_ref[0], query, (), key_all, value_ext, out_ref, (), total_ref
    )


def attend(packed, valid, heads):
    count = packed.shape[0]
    width = min(256, count)
    span = min(512, count)
    return pl.pallas_call(
        functools.partial(attend_kernel, heads, width, span),
        grid_spec=pltpu.PrefetchScalarGridSpec(
            num_scalar_prefetch=1,
            grid=(count // width,),
            in_specs=[pl.BlockSpec((count, (heads + 2) * HD), lambda i, _: (0, 0))],
            out_specs=pl.BlockSpec((width, heads * HD), lambda i, _: (i, 0)),
            scratch_shapes=[
                pltpu.VMEM((count, HD), jnp.bfloat16),
                pltpu.VMEM((count, 2 * HD), jnp.bfloat16),
                pltpu.VMEM((heads * width, 2 * HD), jnp.float32),
            ],
        ),
        out_shape=jax.ShapeDtypeStruct((count, heads * HD), jnp.bfloat16),
        cost_estimate=pl.CostEstimate(
            flops=4 * heads * count * count * HD,
            bytes_accessed=2 * count * HD * (2 * heads + 2),
            transcendentals=heads * count * count,
        ),
        compiler_params=pltpu.CompilerParams(
            dimension_semantics=("arbitrary",), vmem_limit_bytes=40 * 1024 * 1024
        ),
    )(valid, packed)


def exchange(array):
    return lax.all_to_all(
        array, "tp", split_axis=0, concat_axis=0, tiled=True
    )


def per_device(queries, keys, values, lengths):
    seqs, rows, _ = queries.shape
    devices = lax.axis_size("tp")
    count = devices * rows
    if fused_fits(devices):
        return fused_by_length(queries, keys, values, lengths)

    pairs = seqs * HEADS
    owned = pairs // devices
    heads_q = queries.reshape(seqs, rows, HEADS, HD)
    heads_k = jnp.repeat(keys.reshape(seqs, rows, KVH, HD), GROUP, axis=2)
    heads_v = jnp.repeat(values.reshape(seqs, rows, KVH, HD), GROUP, axis=2)
    packed = jnp.concatenate([heads_q, heads_k, heads_v], axis=3)
    packed = packed.transpose(0, 2, 1, 3).reshape(devices, owned * rows, 3 * HD)
    gathered = exchange(packed).reshape(devices, owned, rows, 3 * HD)
    outs = []
    for o in range(owned):
        seq = (lax.axis_index("tp") * owned + o) // HEADS
        valid = jnp.sum(jnp.where(jnp.arange(seqs) == seq, lengths, 0))[None]
        outs.append(attend(gathered[:, o].reshape(count, 3 * HD), valid, 1))
    output = jnp.stack(outs).reshape(owned, devices, rows, HD).transpose(1, 0, 2, 3)
    returned = exchange(output.reshape(devices, owned * rows, HD))
    return (
        returned.reshape(seqs, HEADS, rows, HD)
        .transpose(0, 2, 1, 3)
        .reshape(seqs, rows, HEADS * HD)
    )


def solution(mesh):
    placed = (
        P("groups", "tp", None),
        P("groups", "tp", None),
        P("groups", "tp", None),
        P("groups"),
    )
    return jax.shard_map(
        per_device, mesh=mesh, in_specs=placed, out_specs=P("groups", "tp", None), check_vma=False
    )
```
